32 devices in a mesh: groups: 2 (over y), seq: 4 (over z), head: 4 (over x, core).
Axes of the slice: x: 2, y: 2, z: 4, core: 2. Of those that a mesh axis runs over, the one named last changes fastest.
Arguments:
- queries: bfloat16 [32, 3, 32, 128], P('groups', None, 'head'), parts along dimension 0, may hold values from -8 to 8
- new_kv: bfloat16 [4, 16, 3, 4, 128], P('groups', None, None, 'head'), parts along dimension 0, may hold values from -16 to 16
- res_kv: bfloat16 [4, 2, 16384, 4, 128], P('groups', None, 'seq', 'head'), parts along dimension 0, may hold values from -16 to 16
- prefill_kv: bfloat16 [4, 4, 4096, 128], P('groups', None, ('seq', 'head')), parts along dimension 0, may hold values from -16 to 16
- block_table: int32 [128], P('groups'), parts along dimension 0, may hold values from 0 to 63, as said below
- lengths: int32 [6], P('groups'), parts along dimension 0, may hold values from 4096 to 16384, as said below
- join_step: int32 [2], P('groups'), parts along dimension 0, may hold values from 1 to 15
Outputs:
- attn_out: bfloat16 [32, 3, 32, 128], P('groups', None, 'head'), parts along dimension 0
- new_cache: bfloat16 [4, 4, 4096, 128], P('groups', 'head', 'seq'), parts along dimension 0
The draws below stay inside these ranges and needn't reach their ends.
There are 2 independent parts, one for each index of `groups`. The reference program is written for one: setup_inputs(seed, part) draws one part's arguments, and reference() takes and returns one part's arrays. A program takes and returns all parts, laid end to end along the dimension named above; each array names one. Nothing has to cross between parts.
Inputs may be any that keep to these rules, and one draw needn't show every extreme that they name: `block_table`: A permutation of 0 to 63. In each aligned run of 4 entries (the blocks of one prefill device) every aligned range of 16 slots is named exactly 1 times. `lengths`: entries 0 to 1 lie between 4096 and 16384, and one of them equals 16384; entry 2 equals 4096.
All inputs are finite; a program needn't handle non-finite values.
Results may differ from the reference program's by a relative error of at most 0.0039.
Values may be sent and summed in bfloat16 or wider, within the bound.
A program may use at most 64 MiB of HBM per device.

```python
import math
import jax
import jax.numpy as jnp
from jax import lax

HD = 128
QPK = 8
RES = 2
STEPS = 16
BLOCK = 64
PAGES = 1
KVH = 4
QH = 32
DEV_BLOCKS = 4
LNEW = 4096
NBLK = 64
RES_LEN = 16384


def query_values(key):
    array_shape = (STEPS, RES + 1, QH, HD)
    base_draw = jax.random.normal(jax.random.fold_in(key, 31), array_shape, jnp.float32)
    return jnp.clip(base_draw, -8.0, 8.0)


def draw_queries(key, part):
    return query_values(key).astype(jnp.bfloat16)


def draw_new_kv(key, part):
    array_shape = (STEPS, RES + 1, KVH, HD)
    centre = query_values(key).reshape(STEPS, RES + 1, KVH, QPK, HD).mean(axis=3)
    key_part = 9.0 * centre + 1.5 * jax.random.normal(jax.random.fold_in(key, 51), array_shape, jnp.float32)
    value_part = jax.random.normal(jax.random.fold_in(key, 52), array_shape, jnp.float32)
    return jnp.clip(jnp.stack([key_part, value_part]), -16.0, 16.0).astype(jnp.bfloat16)


def draw_res_kv(key, part):
    array_shape = (RES, RES_LEN, KVH, HD)
    key_part = 3.0 * jax.random.normal(jax.random.fold_in(key, 11), array_shape, jnp.float32)
    value_part = jax.random.normal(jax.random.fold_in(key, 12), array_shape, jnp.float32)
    return jnp.clip(jnp.stack([key_part, value_part]), -16.0, 16.0).astype(jnp.bfloat16)


def draw_prefill_kv(key, part):
    array_shape = (KVH, LNEW, HD)
    key_part = 3.0 * jax.random.normal(jax.random.fold_in(key, 13), array_shape, jnp.float32)
    value_part = jax.random.normal(jax.random.fold_in(key, 14), array_shape, jnp.float32)
    return jnp.clip(jnp.stack([key_part, value_part]), -16.0, 16.0).astype(jnp.bfloat16)


def shuffle_pattern(sub_key, pattern):
    return jax.random.permutation(sub_key, pattern)


def draw_block_table(key, part):
    shard_count = DEV_BLOCKS // PAGES
    sender_count = NBLK // DEV_BLOCKS
    pattern = jnp.repeat(jnp.arange(shard_count, dtype=jnp.int32), PAGES)
    sender_keys = jax.random.split(jax.random.fold_in(key, 41), sender_count)
    shard_of = jax.vmap(shuffle_pattern, in_axes=(0, None))(sender_keys, pattern).reshape(-1).astype(jnp.int32)
    priority = jax.random.permutation(jax.random.fold_in(key, 42), NBLK).astype(jnp.int32)
    ordering = jnp.argsort(shard_of * NBLK + priority, stable=True).astype(jnp.int32)
    return jnp.zeros((NBLK,), jnp.int32).at[ordering].set(jnp.arange(NBLK, dtype=jnp.int32))


def draw_lengths(key, part):
    resident = jax.random.randint(jax.random.fold_in(key, 61), (RES,), RES_LEN // 4, RES_LEN + 1)
    full_one = jax.random.randint(jax.random.fold_in(key, 63), (), 0, RES)
    resident = jnp.where(jnp.arange(RES, dtype=jnp.int32) == full_one, RES_LEN, resident)
    joining = jnp.full((1,), LNEW, jnp.int32)
    return jnp.concatenate([resident.astype(jnp.int32), joining]).astype(jnp.int32)


def setup_inputs(seed: int = 0, part: int = 0) -> dict:
    key_of = jax.random.split(jax.random.key(seed), 8)
    part_keys = jax.random.split(jax.random.fold_in(key_of[7], part), 8)
    return {
        "queries": draw_queries(jax.random.fold_in(jax.random.fold_in(key_of[7], part), 71), part),
        "new_kv": draw_new_kv(jax.random.fold_in(jax.random.fold_in(key_of[7], part), 71), part),
        "res_kv": draw_res_kv(jax.random.fold_in(jax.random.fold_in(key_of[7], part), 71), part),
        "prefill_kv": draw_prefill_kv(jax.random.fold_in(jax.random.fold_in(key_of[7], part), 71), part),
        "block_table": draw_block_table(jax.random.fold_in(jax.random.fold_in(key_of[7], part), 71), part),
        "lengths": draw_lengths(jax.random.fold_in(jax.random.fold_in(key_of[7], part), 71), part),
        "join_step": jax.random.randint(part_keys[6], (1,), 1, STEPS).astype(jnp.int32),
    }


def attend(query_rows, head_keys, head_values, valid_mask, fresh_keys, fresh_values, fresh_valid):
    score_scale = 1.0 / math.sqrt(HD)
    highest = lax.Precision.HIGHEST

    def per_head(operands):
        rows_here, keys_here, values_here, new_keys, new_values = operands
        rows_wide = rows_here.astype(jnp.float32)
        cache_scores = jnp.einsum('sqd,ld->sql', rows_wide, keys_here.astype(jnp.float32), precision=highest) * score_scale
        cache_scores = jnp.where(valid_mask[None, None, :], cache_scores, -jnp.inf)
        fresh_scores = jnp.einsum('sqd,ud->squ', rows_wide, new_keys.astype(jnp.float32), precision=highest) * score_scale
        fresh_scores = jnp.where(fresh_valid[:, None, :], fresh_scores, -jnp.inf)
        row_max = jnp.maximum(lax.optimization_barrier(jnp.max(cache_scores, axis=-1)), lax.optimization_barrier(jnp.max(fresh_scores, axis=-1)))
        cache_weight = jnp.exp(cache_scores - row_max[..., None])
        fresh_weight = jnp.exp(fresh_scores - row_max[..., None])
        row_total = lax.optimization_barrier(jnp.sum(cache_weight, axis=-1)) + lax.optimization_barrier(jnp.sum(fresh_weight, axis=-1))
        cache_round = lax.optimization_barrier(cache_weight.astype(jnp.bfloat16)).astype(jnp.float32)
        fresh_round = lax.optimization_barrier(fresh_weight.astype(jnp.bfloat16)).astype(jnp.float32)
        summed = jnp.einsum('sql,ld->sqd', cache_round, values_here.astype(jnp.float32), precision=highest)
        summed = summed + jnp.einsum('squ,ud->sqd', fresh_round, new_values.astype(jnp.float32), precision=highest)
        return summed / row_total[..., None]
    answer = lax.map(per_head, (jnp.transpose(query_rows, (1, 0, 2, 3)), head_keys, head_values, jnp.transpose(fresh_keys, (1, 0, 2)), jnp.transpose(fresh_values, (1, 0, 2))))
    return jnp.transpose(answer, (1, 0, 2, 3)).reshape(STEPS, KVH * QPK, HD)

def reference(queries, new_kv, res_kv, prefill_kv, block_table, lengths, join_step):
    joined = join_step[0]
    step_ids = jnp.arange(STEPS, dtype=jnp.int32)
    earlier = step_ids[None, :] <= step_ids[:, None]
    answers = []
    for request in range(RES):
        valid_mask = jnp.arange(RES_LEN, dtype=jnp.int32) < lengths[request]
        query_rows = queries[:, request].reshape(STEPS, KVH, QPK, HD)
        head_keys = jnp.moveaxis(res_kv[0, request], 1, 0)
        head_values = jnp.moveaxis(res_kv[1, request], 1, 0)
        answers.append(attend(query_rows, head_keys, head_values, valid_mask, new_kv[0, :, request], new_kv[1, :, request], earlier))
    valid_mask = jnp.arange(LNEW, dtype=jnp.int32) < lengths[RES]
    query_rows = queries[:, RES].reshape(STEPS, KVH, QPK, HD)
    fresh_valid = earlier & (step_ids[None, :] >= joined)
    joining = attend(query_rows, prefill_kv[0], prefill_kv[1], valid_mask, new_kv[0, :, RES], new_kv[1, :, RES], fresh_valid)
    joining = jnp.where((step_ids >= joined)[:, None, None], joining, 0.0)
    attn_out = jnp.stack(answers + [joining], axis=1).astype(jnp.bfloat16)
    blocks = prefill_kv.reshape(2, KVH, NBLK, BLOCK, HD)
    new_cache = jnp.zeros_like(blocks).at[:, :, block_table].set(blocks).reshape(2, KVH, LNEW, HD)
    return (attn_out, new_cache)
```

```python
import functools
import math

import jax
import jax.numpy as jnp
from jax import lax
from jax.experimental import pallas as pl
from jax.experimental.pallas import tpu as pltpu
from jax.sharding import PartitionSpec as P

very_low = -1e30
MESH = pl.DeviceIdType.MESH
NT = (((1,), (1,)), ((), ()))
TN = (((0,), (0,)), ((), ()))


def kernel(
    seq_count,
    head_count,
    queries,
    fresh,
    prefill,
    table,
    lengths,
    join_step,
    res_kv,
    attn_out,
    new_cache,
    res_buf,
    staged,
    arrived,
    own_acc,
    own_stat,
    fresh_acc,
    fresh_stat,
    out_acc,
    out_stat,
    got_acc,
    got_stat,
    slot_of,
    base_of,
    res_sem,
    block_sems,
    acc_send,
    acc_recv,
    stat_send,
    stat_recv,
):
    seq_index = lax.axis_index("seq")
    head_index = lax.axis_index("head")
    senders = seq_count * head_count
    me = seq_index * head_count + head_index
    step_count, request_count, group_size, head_dim = queries.shape
    rows = step_count * group_size
    resident = res_kv.shape[1]
    res_rows = res_kv.shape[2]
    dev_blocks, block_len = prefill.shape[2], prefill.shape[3]
    slot_count = senders * dev_blocks // seq_count
    scale = 1.0 / math.sqrt(head_dim)
    joined = join_step[0]

    barrier = pltpu.get_barrier_semaphore()

    def greet(o, _):
        peer = lax.rem(me + o, senders)
        pl.semaphore_signal(
            barrier,
            inc=1,
            device_id={"seq": peer // head_count, "head": lax.rem(peer, head_count)},
            device_id_type=MESH,
        )
        return 0

    lax.fori_loop(1, senders, greet, 0)

    res_copies = []
    for r in range(resident):
        for c in range(2):
            copy = pltpu.make_async_copy(res_kv.at[c, r], res_buf.at[c, r], res_sem.at[c, r])
            copy.start()
            res_copies.append(copy)

    def block_for(sender, shard):
        found = jnp.int32(0)
        slot = jnp.int32(0)
        for k in range(dev_blocks):
            here = table[sender * dev_blocks + k]
            hit = (here // slot_count) == shard
            found = jnp.where(hit, k, found)
            slot = jnp.where(hit, here, slot)
        return found, slot

    def stage(z, _):
        found, _slot = block_for(me, z)
        for h in range(head_count):
            for c in range(2):
                staged[z * head_count + h, c] = prefill[c, h, found]
        return 0

    lax.fori_loop(0, seq_count, stage, 0)
    pl.semaphore_wait(barrier, senders - 1)

    def send(o, _):
        peer = lax.rem(me + o, senders)
        pltpu.make_async_remote_copy(
            src_ref=staged.at[peer],
            dst_ref=arrived.at[me],
            send_sem=block_sems.at[0],
            recv_sem=block_sems.at[1],
            device_id={"seq": peer // head_count, "head": lax.rem(peer, head_count)},
            device_id_type=MESH,
        ).start()
        return 0

    lax.fori_loop(1, senders, send, 0)
    arrived[me] = staged[me]

    def locate(s, _):
        found, slot = block_for(s, seq_index)
        slot_of[s] = slot - seq_index * slot_count
        base_of[s] = (s * dev_blocks + found) * block_len
        return 0

    lax.fori_loop(0, senders, locate, 0)

    def query_rows(r):
        wide = queries[:, r].astype(jnp.float32).reshape(rows, head_dim)
        return wide.astype(jnp.bfloat16)

    def fold(carry, keys, values, valid, q):
        m, l, acc = carry
        s = lax.dot_general(keys, q, NT, preferred_element_type=jnp.float32) * scale
        s = jnp.where(valid, s, very_low)
        top = jnp.maximum(m, jnp.max(s, axis=0, keepdims=True))
        w = jnp.where(valid, jnp.exp(s - top), 0.0)
        keep = jnp.exp(m - top)
        l = l * keep + jnp.sum(w, axis=0, keepdims=True)
        acc = acc * keep + lax.dot_general(
            values, w.astype(jnp.bfloat16), TN, preferred_element_type=jnp.float32
        )
        return top, l, acc

    empty = (
        jnp.full((1, rows), very_low, jnp.float32),
        jnp.zeros((1, rows), jnp.float32),
        jnp.zeros((head_dim, rows), jnp.float32),
    )

    chunk = math.gcd(res_rows, 1024)
    for r in range(resident):
        q = query_rows(r)
        res_copies[2 * r].wait()
        res_copies[2 * r + 1].wait()
        limit = lengths[r] - seq_index * res_rows

        def step(i, carry, r=r, q=q, limit=limit):
            at = pl.ds(pl.multiple_of(i * chunk, chunk), chunk)
            valid = lax.broadcasted_iota(jnp.int32, (chunk, rows), 0) + i * chunk < limit
            return fold(carry, res_buf[0, r, at], res_buf[1, r, at], valid, q)

        m, l, acc = lax.fori_loop(0, res_rows // chunk, step, empty)
        own_stat[2 * r : 2 * r + 1] = m
        own_stat[2 * r + 1 : 2 * r + 2] = l
        own_acc[r] = acc
        out_acc[r] = acc.astype(jnp.bfloat16)
        out_stat[0, 2 * r : 2 * r + 1] = m
        out_stat[0, 2 * r + 1 : 2 * r + 2] = l

    when = lax.broadcasted_iota(jnp.int32, (step_count, rows), 1) // group_size
    which = lax.broadcasted_iota(jnp.int32, (step_count, rows), 0)
    for r in range(request_count):
        allowed = which <= when
        if r >= resident:
            allowed = allowed & (which >= joined)
        m, l, acc = fold(empty, fresh[0, r], fresh[1, r], allowed, query_rows(r))
        fresh_stat[2 * r : 2 * r + 1] = m
        fresh_stat[2 * r + 1 : 2 * r + 2] = l
        fresh_acc[r] = acc

    def push(phase, first, count):
        for o in range(1, seq_count):
            peer = lax.rem(seq_index + o, seq_count)
            pltpu.make_async_remote_copy(
                src_ref=out_acc.at[pl.ds(first, count)],
                dst_ref=got_acc.at[seq_index, pl.ds(first, count)],
                send_sem=acc_send.at[phase],
                recv_sem=acc_recv.at[phase],
                device_id={"seq": peer},
                device_id_type=MESH,
            ).start()
            pltpu.make_async_remote_copy(
                src_ref=out_stat.at[phase],
                dst_ref=got_stat.at[seq_index, phase],
                send_sem=stat_send.at[phase],
                recv_sem=stat_recv.at[phase],
                device_id={"seq": peer},
                device_id_type=MESH,
            ).start()

    def drain(acc_sem, stat_sem, phase, first, count):
        part = got_acc.at[pl.ds(0, seq_count - 1), pl.ds(first, count)]
        pltpu.make_async_copy(part, part, acc_sem.at[phase]).wait()
        part = got_stat.at[pl.ds(0, seq_count - 1), phase]
        pltpu.make_async_copy(part, part, stat_sem.at[phase]).wait()

    push(0, 0, resident)

    part = arrived.at[pl.ds(0, senders - 1)]
    pltpu.make_async_copy(part, part, block_sems.at[1]).wait()

    q = query_rows(resident)
    some = math.gcd(senders, 16)

    def step(i, carry):
        first = i * some
        keys = arrived[pl.ds(first, some), 0].reshape(some * block_len, head_dim)
        values = arrived[pl.ds(first, some), 1].reshape(some * block_len, head_dim)
        offsets = lax.broadcasted_iota(jnp.int32, (block_len, rows), 0)
        positions = jnp.concatenate([offsets + base_of[first + s] for s in range(some)], axis=0)
        return fold(carry, keys, values, positions < lengths[resident], q)

    m, l, acc = lax.fori_loop(0, senders // some, step, empty)
    out_acc[resident] = acc.astype(jnp.bfloat16)
    out_stat[1, 0:1] = m
    out_stat[1, 1:2] = l
    own_stat[2 * resident : 2 * resident + 1] = m
    own_stat[2 * resident + 1 : 2 * resident + 2] = l
    own_acc[resident] = acc
    push(1, resident, 1)

    def place(j, _):
        def look(s, found):
            return jnp.where(slot_of[s] == j, s, found)

        source = lax.fori_loop(0, senders, look, jnp.int32(0), unroll=math.gcd(senders, 16))
        at = pl.ds(pl.multiple_of(j * block_len, block_len), block_len)
        for c in range(2):
            new_cache[c, 0, at] = arrived[source, c]
        return 0

    lax.fori_loop(0, slot_count, place, 0)

    def finish(r, phase, row):
        peers = [lax.rem(seq_index + o, seq_count) for o in range(1, seq_count)]
        maxima = [own_stat[2 * r : 2 * r + 1], fresh_stat[2 * r : 2 * r + 1]]
        totals = [own_stat[2 * r + 1 : 2 * r + 2], fresh_stat[2 * r + 1 : 2 * r + 2]]
        for peer in peers:
            maxima.append(got_stat[peer, phase, row : row + 1])
            totals.append(got_stat[peer, phase, row + 1 : row + 2])
        top = functools.reduce(jnp.maximum, maxima)
        factors = [jnp.exp(m - top) for m in maxima]
        total = sum(f * t for f, t in zip(factors, totals))
        summed = own_acc[r] * factors[0] + fresh_acc[r] * factors[1]
        for peer, f in zip(peers, factors[2:]):
            summed = summed + got_acc[peer, r].astype(jnp.float32) * f
        if r >= resident:
            lane = lax.broadcasted_iota(jnp.int32, (head_dim, rows), 1) // group_size
            summed = jnp.where(lane >= joined, summed / total, 0.0)
        else:
            summed = summed / total
        result = jnp.transpose(summed).reshape(step_count, group_size, head_dim)
        attn_out[:, r] = result.astype(jnp.bfloat16)

    drain(acc_recv, stat_recv, 0, 0, resident)
    for r in range(resident):
        finish(r, 0, 2 * r)
    drain(acc_recv, stat_recv, 1, resident, 1)
    finish(resident, 1, 0)

    part = staged.at[pl.ds(0, senders - 1)]
    pltpu.make_async_copy(part, part, block_sems.at[0]).wait()
    drain(acc_send, stat_send, 0, 0, resident)
    drain(acc_send, stat_send, 1, resident, 1)


def per_device(seq_count, head_count, queries, new_kv, res_kv, prefill_kv, block_table, lengths, join_step):
    step_count, request_count, group_size, head_dim = queries.shape
    rows = step_count * group_size
    resident, res_rows = res_kv.shape[1], res_kv.shape[2]
    head_total, new_rows = prefill_kv.shape[1], prefill_kv.shape[2]
    senders = seq_count * head_count
    dev_blocks = block_table.shape[0] // senders
    block_len = new_rows // dev_blocks
    if dev_blocks != seq_count or resident > 4 or head_total != head_count:
        raise ValueError("unsupported sizes")
    slot_count = block_table.shape[0] // seq_count
    fresh = jnp.transpose(new_kv[:, :, :, 0], (0, 2, 1, 3))
    prefill = prefill_kv.reshape(2, head_total, dev_blocks, block_len, head_dim)
    vmem = pl.BlockSpec(memory_space=pltpu.VMEM)
    smem = pl.BlockSpec(memory_space=pltpu.SMEM)
    bf16, f32 = jnp.bfloat16, jnp.float32
    return pl.pallas_call(
        functools.partial(kernel, seq_count, head_count),
        out_shape=(
            jax.ShapeDtypeStruct(queries.shape, bf16),
            jax.ShapeDtypeStruct((2, 1, slot_count * block_len, head_dim), bf16),
        ),
        in_specs=[vmem, vmem, vmem, smem, smem, smem, pl.BlockSpec(memory_space=pl.ANY)],
        out_specs=(vmem, vmem),
        scratch_shapes=[
            pltpu.VMEM((2, resident, res_rows, head_dim), bf16),
            pltpu.VMEM((senders, 2, block_len, head_dim), bf16),
            pltpu.VMEM((senders, 2, block_len, head_dim), bf16),
            pltpu.VMEM((request_count, head_dim, rows), f32),
            pltpu.VMEM((16, rows), f32),
            pltpu.VMEM((request_count, head_dim, rows), f32),
            pltpu.VMEM((16, rows), f32),
            pltpu.VMEM((request_count, head_dim, rows), bf16),
            pltpu.VMEM((2, 8, rows), f32),
            pltpu.VMEM((seq_count, request_count, head_dim, rows), bf16),
            pltpu.VMEM((seq_count, 2, 8, rows), f32),
            pltpu.SMEM((senders,), jnp.int32),
            pltpu.SMEM((senders,), jnp.int32),
            pltpu.SemaphoreType.DMA((2, resident)),
            pltpu.SemaphoreType.DMA((2,)),
            pltpu.SemaphoreType.DMA((2,)),
            pltpu.SemaphoreType.DMA((2,)),
            pltpu.SemaphoreType.DMA((2,)),
            pltpu.SemaphoreType.DMA((2,)),
        ],
        compiler_params=pltpu.CompilerParams(collective_id=0, has_side_effects=True),
    )(
        queries,
        fresh,
        prefill,
        block_table,
        lengths,
        join_step,
        res_kv.reshape(2, resident, res_rows, head_dim),
    )


def solution(mesh):
    in_specs = (
        P("groups", None, "head", None),
        P("groups", None, None, "head", None),
        P("groups", None, "seq", "head", None),
        P("groups", None, ("seq", "head"), None),
        P("groups"),
        P("groups"),
        P("groups"),
    )
    out_specs = (P("groups", None, "head", None), P("groups", "head", "seq", None))
    body = functools.partial(per_device, mesh.shape["seq"], mesh.shape["head"])
    return jax.shard_map(body, mesh=mesh, in_specs=in_specs, out_specs=out_specs, check_vma=False)
```

```python
import functools
import math

import jax
import jax.numpy as jnp
from jax import lax
from jax.experimental import pallas as pl
from jax.experimental.pallas import tpu as pltpu
from jax.sharding import PartitionSpec as P

very_low = -1e30
MESH = pl.DeviceIdType.MESH
NT = (((1,), (1,)), ((), ()))
TN = (((0,), (0,)), ((), ()))


def kernel(
    seq_count,
    head_count,
    queries,
    fresh,
    prefill_kv,
    table,
    lengths,
    join_step,
    res_kv,
    attn_out,
    new_cache,
    prefill,
    res_buf,
    staged,
    arrived,
    own_acc,
    own_stat,
    fresh_acc,
    fresh_stat,
    out_acc,
    out_stat,
    got_acc,
    got_stat,
    slice_send,
    slice_got,
    whole_out,
    slot_of,
    base_of,
    prefill_sem,
    res_sem,
    block_sems,
    acc_send,
    acc_recv,
    stat_send,
    stat_recv,
    slice_sems,
    whole_sems,
):
    seq_index = lax.axis_index("seq")
    head_index = lax.axis_index("head")
    senders = seq_count * head_count
    me = seq_index * head_count + head_index
    step_count, request_count, group_size, head_dim = queries.shape
    rows = step_count * group_size
    resident = res_kv.shape[1]
    res_rows = res_kv.shape[2]
    dev_blocks, block_len = prefill.shape[2], prefill.shape[3]
    slot_count = senders * dev_blocks // seq_count
    scale = 1.0 / math.sqrt(head_dim)
    joined = join_step[0]
    part_dim = head_dim // seq_count
    peers = [lax.rem(seq_index + o, seq_count) for o in range(1, seq_count)]

    fetch = pltpu.make_async_copy(prefill_kv, prefill, prefill_sem)
    fetch.start()
    barrier = pltpu.get_barrier_semaphore()

    def greet(o, _):
        peer = lax.rem(me + o, senders)
        pl.semaphore_signal(
            barrier,
            inc=1,
            device_id={"seq": peer // head_count, "head": lax.rem(peer, head_count)},
            device_id_type=MESH,
        )
        return 0

    lax.fori_loop(1, senders, greet, 0)

    res_copies = []
    for r in range(resident):
        for c in range(2):
            copy = pltpu.make_async_copy(res_kv.at[c, r], res_buf.at[c, r], res_sem.at[c, r])
            copy.start()
            res_copies.append(copy)

    def block_for(sender, shard):
        found = jnp.int32(0)
        slot = jnp.int32(0)
        for k in range(dev_blocks):
            here = table[sender * dev_blocks + k]
            hit = (here // slot_count) == shard
            found = jnp.where(hit, k, found)
            slot = jnp.where(hit, here, slot)
        return found, slot

    def stage(z, _):
        found, _slot = block_for(me, z)
        for h in range(head_count):
            for c in range(2):
                staged[z * head_count + h, c] = prefill[c, h, found]
        return 0

    fetch.wait()
    lax.fori_loop(0, seq_count, stage, 0)
    pl.semaphore_wait(barrier, senders - 1)

    def send(o, _):
        peer = lax.rem(me + o, senders)
        pltpu.make_async_remote_copy(
            src_ref=staged.at[peer],
            dst_ref=arrived.at[me],
            send_sem=block_sems.at[0],
            recv_sem=block_sems.at[1],
            device_id={"seq": peer // head_count, "head": lax.rem(peer, head_count)},
            device_id_type=MESH,
        ).start()
        return 0

    lax.fori_loop(1, senders, send, 0)
    arrived[me] = staged[me]

    def locate(s, _):
        found, slot = block_for(s, seq_index)
        slot_of[s] = slot - seq_index * slot_count
        base_of[s] = (s * dev_blocks + found) * block_len
        return 0

    lax.fori_loop(0, senders, locate, 0)

    def query_rows(r):
        wide = queries[:, r].astype(jnp.float32).reshape(rows, head_dim)
        return wide.astype(jnp.bfloat16)

    def fold(carry, keys, values, valid, q):
        m, l, acc = carry
        s = lax.dot_general(keys, q, NT, preferred_element_type=jnp.float32) * scale
        s = jnp.where(valid, s, very_low)
        top = jnp.maximum(m, jnp.max(s, axis=0, keepdims=True))
        w = jnp.where(valid, jnp.exp(s - top), 0.0)
        keep = jnp.exp(m - top)
        l = l * keep + jnp.sum(w, axis=0, keepdims=True)
        acc = acc * keep + lax.dot_general(
            values, w.astype(jnp.bfloat16), TN, preferred_element_type=jnp.float32
        )
        return top, l, acc

    empty = (
        jnp.full((1, rows), very_low, jnp.float32),
        jnp.zeros((1, rows), jnp.float32),
        jnp.zeros((head_dim, rows), jnp.float32),
    )

    chunk = math.gcd(res_rows, 1024)
    for r in range(resident):
        q = query_rows(r)
        res_copies[2 * r].wait()
        res_copies[2 * r + 1].wait()
        limit = lengths[r] - seq_index * res_rows

        def step(i, carry, r=r, q=q, limit=limit):
            at = pl.ds(pl.multiple_of(i * chunk, chunk), chunk)
            valid = lax.broadcasted_iota(jnp.int32, (chunk, rows), 0) + i * chunk < limit
            return fold(carry, res_buf[0, r, at], res_buf[1, r, at], valid, q)

        m, l, acc = lax.fori_loop(0, res_rows // chunk, step, empty)
        own_stat[2 * r : 2 * r + 1] = m
        own_stat[2 * r + 1 : 2 * r + 2] = l
        own_acc[r] = acc
        pieces = acc.reshape(seq_count, part_dim, rows).astype(jnp.bfloat16)
        for z in range(seq_count):
            slice_send[z, r] = pieces[z]
        out_stat[0, 2 * r : 2 * r + 1] = m
        out_stat[0, 2 * r + 1 : 2 * r + 2] = l

    when = lax.broadcasted_iota(jnp.int32, (step_count, rows), 1) // group_size
    which = lax.broadcasted_iota(jnp.int32, (step_count, rows), 0)
    for r in range(request_count):
        allowed = which <= when
        if r >= resident:
            allowed = allowed & (which >= joined)
        m, l, acc = fold(empty, fresh[0, r], fresh[1, r], allowed, query_rows(r))
        fresh_stat[2 * r : 2 * r + 1] = m
        fresh_stat[2 * r + 1 : 2 * r + 2] = l
        fresh_acc[r] = acc

    def remote(source, target, send_sem, recv_sem, peer):
        pltpu.make_async_remote_copy(
            src_ref=source,
            dst_ref=target,
            send_sem=send_sem,
            recv_sem=recv_sem,
            device_id={"seq": peer},
            device_id_type=MESH,
        ).start()

    def drain(buffer, sem):
        part = buffer.at[pl.ds(0, seq_count - 1)]
        pltpu.make_async_copy(part, part, sem).wait()

    def push_stat(phase):
        for peer in peers:
            remote(
                out_stat.at[phase],
                got_stat.at[phase, seq_index],
                stat_send.at[phase],
                stat_recv.at[phase],
                peer,
            )

    def merge(r, phase, row, own, new, got):
        maxima = [own_stat[2 * r : 2 * r + 1], fresh_stat[2 * r : 2 * r + 1]]
        totals = [own_stat[2 * r + 1 : 2 * r + 2], fresh_stat[2 * r + 1 : 2 * r + 2]]
        for peer in peers:
            maxima.append(got_stat[phase, peer, row : row + 1])
            totals.append(got_stat[phase, peer, row + 1 : row + 2])
        top = functools.reduce(jnp.maximum, maxima)
        factors = [jnp.exp(m - top) for m in maxima]
        total = sum(f * t for f, t in zip(factors, totals))
        summed = own * factors[0] + new * factors[1]
        for peer, f in zip(peers, factors[2:]):
            summed = summed + got(peer).astype(jnp.float32) * f
        return summed / total

    push_stat(0)
    for peer in peers:
        remote(slice_send.at[peer], slice_got.at[seq_index], slice_sems.at[0], slice_sems.at[1], peer)

    drain(got_stat.at[0], stat_recv.at[0])
    drain(slice_got, slice_sems.at[1])
    mine = pl.ds(pl.multiple_of(seq_index * part_dim, part_dim), part_dim)
    for r in range(resident):
        whole_out[seq_index, r] = merge(
            r, 0, 2 * r, own_acc[r, mine], fresh_acc[r, mine], lambda peer: slice_got[peer, r]
        ).astype(jnp.bfloat16)
    for peer in peers:
        remote(
            whole_out.at[seq_index], whole_out.at[seq_index], whole_sems.at[0], whole_sems.at[1], peer
        )

    part = arrived.at[pl.ds(0, senders - 1)]
    pltpu.make_async_copy(part, part, block_sems.at[1]).wait()

    q = query_rows(resident)
    some = math.gcd(senders, 16)

    def step(i, carry):
        first = i * some
        keys = arrived[pl.ds(first, some), 0].reshape(some * block_len, head_dim)
        values = arrived[pl.ds(first, some), 1].reshape(some * block_len, head_dim)
        offsets = lax.broadcasted_iota(jnp.int32, (block_len, rows), 0)
        positions = jnp.concatenate([offsets + base_of[first + s] for s in range(some)], axis=0)
        return fold(carry, keys, values, positions < lengths[resident], q)

    m, l, acc = lax.fori_loop(0, senders // some, step, empty)
    out_acc[...] = acc.astype(jnp.bfloat16)
    out_stat[1, 0:1] = m
    out_stat[1, 1:2] = l
    own_stat[2 * resident : 2 * resident + 1] = m
    own_stat[2 * resident + 1 : 2 * resident + 2] = l
    own_acc[resident] = acc
    push_stat(1)
    for peer in peers:
        remote(out_acc, got_acc.at[seq_index], acc_send, acc_recv, peer)

    def place(j, _):
        def look(s, found):
            return jnp.where(slot_of[s] == j, s, found)

        source = lax.fori_loop(0, senders, look, jnp.int32(0), unroll=math.gcd(senders, 16))
        at = pl.ds(pl.multiple_of(j * block_len, block_len), block_len)
        for c in range(2):
            new_cache[c, 0, at] = arrived[source, c]
        return 0

    lax.fori_loop(0, slot_count, place, 0)

    def finish(r, result):
        result = jnp.transpose(result).reshape(step_count, group_size, head_dim)
        attn_out[:, r] = result.astype(jnp.bfloat16)

    drain(whole_out, whole_sems.at[1])
    for r in range(resident):
        pieces = [whole_out[z, r].astype(jnp.float32) for z in range(seq_count)]
        finish(r, jnp.concatenate(pieces, axis=0))
    drain(got_stat.at[1], stat_recv.at[1])
    drain(got_acc, acc_recv)
    r = resident
    result = merge(r, 1, 0, own_acc[r], fresh_acc[r], lambda peer: got_acc[peer])
    lane = lax.broadcasted_iota(jnp.int32, (head_dim, rows), 1) // group_size
    finish(r, jnp.where(lane >= joined, result, 0.0))

    part = staged.at[pl.ds(0, senders - 1)]
    pltpu.make_async_copy(part, part, block_sems.at[0]).wait()
    drain(got_stat.at[0], stat_send.at[0])
    drain(slice_got, slice_sems.at[0])
    drain(whole_out, whole_sems.at[0])
    drain(got_stat.at[1], stat_send.at[1])
    drain(got_acc, acc_send)


def per_device(seq_count, head_count, queries, new_kv, res_kv, prefill_kv, block_table, lengths, join_step):
    step_count, request_count, group_size, head_dim = queries.shape
    rows = step_count * group_size
    resident, res_rows = res_kv.shape[1], res_kv.shape[2]
    head_total, new_rows = prefill_kv.shape[1], prefill_kv.shape[2]
    senders = seq_count * head_count
    dev_blocks = block_table.shape[0] // senders
    block_len = new_rows // dev_blocks
    if dev_blocks != seq_count or resident > 4 or head_total != head_count:
        raise ValueError("unsupported sizes")
    slot_count = block_table.shape[0] // seq_count
    fresh = jnp.transpose(new_kv[:, :, :, 0], (0, 2, 1, 3))
    prefill = prefill_kv.reshape(2, head_total, dev_blocks, block_len, head_dim)
    part_dim = head_dim // seq_count
    vmem = pl.BlockSpec(memory_space=pltpu.VMEM)
    smem = pl.BlockSpec(memory_space=pltpu.SMEM)
    hbm = pl.BlockSpec(memory_space=pltpu.HBM)
    bf16, f32 = jnp.bfloat16, jnp.float32
    return pl.pallas_call(
        functools.partial(kernel, seq_count, head_count),
        out_shape=(
            pltpu.VMEM(queries.shape, bf16),
            pltpu.VMEM((2, 1, slot_count * block_len, head_dim), bf16),
        ),
        in_specs=[vmem, vmem, hbm, smem, smem, smem, hbm],
        out_specs=(vmem, vmem),
        scratch_shapes=[
            pltpu.VMEM(prefill.shape, bf16),
            pltpu.VMEM((2, resident, res_rows, head_dim), bf16),
            pltpu.VMEM((senders, 2, block_len, head_dim), bf16),
            pltpu.VMEM((senders, 2, block_len, head_dim), bf16),
            pltpu.VMEM((request_count, head_dim, rows), f32),
            pltpu.VMEM((16, rows), f32),
            pltpu.VMEM((request_count, head_dim, rows), f32),
            pltpu.VMEM((16, rows), f32),
            pltpu.VMEM((head_dim, rows), bf16),
            pltpu.VMEM((2, 8, rows), f32),
            pltpu.VMEM((seq_count, head_dim, rows), bf16),
            pltpu.VMEM((2, seq_count, 8, rows), f32),
            pltpu.VMEM((seq_count, resident, part_dim, rows), bf16),
            pltpu.VMEM((seq_count, resident, part_dim, rows), bf16),
            pltpu.VMEM((seq_count, resident, part_dim, rows), bf16),
            pltpu.SMEM((senders,), jnp.int32),
            pltpu.SMEM((senders,), jnp.int32),
            pltpu.SemaphoreType.DMA,
            pltpu.SemaphoreType.DMA((2, resident)),
            pltpu.SemaphoreType.DMA((2,)),
            pltpu.SemaphoreType.DMA,
            pltpu.SemaphoreType.DMA,
            pltpu.SemaphoreType.DMA((2,)),
            pltpu.SemaphoreType.DMA((2,)),
            pltpu.SemaphoreType.DMA((2,)),
            pltpu.SemaphoreType.DMA((2,)),
        ],
        compiler_params=pltpu.CompilerParams(
            collective_id=0, has_side_effects=True, vmem_limit_bytes=48 * 1024 * 1024
        ),
    )(
        queries,
        fresh,
        prefill,
        block_table,
        lengths,
        join_step,
        res_kv.reshape(2, resident, res_rows, head_dim),
    )


def solution(mesh):
    in_specs = (
        P("groups", None, "head", None),
        P("groups", None, None, "head", None),
        P("groups", None, "seq", "head", None),
        P("groups", None, ("seq", "head"), None),
        P("groups"),
        P("groups"),
        P("groups"),
    )
    out_specs = (P("groups", None, "head", None), P("groups", "head", "seq", None))
    body = functools.partial(per_device, mesh.shape["seq"], mesh.shape["head"])
    return jax.shard_map(body, mesh=mesh, in_specs=in_specs, out_specs=out_specs, check_vma=False)
```

```python
import functools
import math

import jax
import jax.numpy as jnp
from jax import lax
from jax.experimental import pallas as pl
from jax.experimental.pallas import tpu as pltpu
from jax.sharding import PartitionSpec as P

very_low = -1e30
MESH = pl.DeviceIdType.MESH
NT = (((1,), (1,)), ((), ()))
TN = (((0,), (0,)), ((), ()))


def kernel(
    seq_count,
    head_count,
    queries,
    fresh,
    prefill_kv,
    table,
    lengths,
    join_step,
    res_kv,
    attn_out,
    new_cache,
    prefill,
    res_buf,
    staged,
    arrived,
    own_acc,
    own_stat,
    fresh_acc,
    fresh_stat,
    out_acc,
    out_stat,
    got_acc,
    got_stat,
    slice_send,
    slice_got,
    whole_out,
    slot_of,
    base_of,
    prefill_sem,
    res_sem,
    block_sems,
    acc_send,
    acc_recv,
    stat_send,
    stat_recv,
    slice_sems,
    whole_sems,
):
    seq_index = lax.axis_index("seq")
    head_index = lax.axis_index("head")
    senders = seq_count * head_count
    me = seq_index * head_count + head_index
    step_count, request_count, group_size, head_dim = queries.shape
    rows = step_count * group_size
    resident = res_kv.shape[1]
    res_rows = res_kv.shape[2]
    dev_blocks, block_len = prefill.shape[2], prefill.shape[3]
    slot_count = senders * dev_blocks // seq_count
    scale = 1.0 / math.sqrt(head_dim)
    joined = join_step[0]
    part_dim = head_dim // seq_count
    peers = [lax.rem(seq_index + o, seq_count) for o in range(1, seq_count)]

    fetch = pltpu.make_async_copy(prefill_kv, prefill, prefill_sem)
    fetch.start()
    barrier = pltpu.get_barrier_semaphore()

    def greet(o, _):
        peer = lax.rem(me + o, senders)
        pl.semaphore_signal(
            barrier,
            inc=1,
            device_id={"seq": peer // head_count, "head": lax.rem(peer, head_count)},
            device_id_type=MESH,
        )
        return 0

    lax.fori_loop(1, senders, greet, 0)

    res_copies = []
    for r in range(resident):
        for c in range(2):
            copy = pltpu.make_async_copy(res_kv.at[c, r], res_buf.at[c, r], res_sem.at[c, r])
            copy.start()
            res_copies.append(copy)

    def block_for(sender, shard):
        found = jnp.int32(0)
        slot = jnp.int32(0)
        for k in range(dev_blocks):
            here = table[sender * dev_blocks + k]
            hit = (here // slot_count) == shard
            found = jnp.where(hit, k, found)
            slot = jnp.where(hit, here, slot)
        return found, slot

    def stage(z, _):
        found, _slot = block_for(me, z)
        for h in range(head_count):
            for c in range(2):
                staged[z * head_count + h, c] = prefill[c, h, found]
        return 0

    fetch.wait()
    lax.fori_loop(0, seq_count, stage, 0)
    pl.semaphore_wait(barrier, senders - 1)

    def send(o, _):
        peer = lax.rem(me + o, senders)
        pltpu.make_async_remote_copy(
            src_ref=staged.at[peer],
            dst_ref=arrived.at[me],
            send_sem=block_sems.at[0],
            recv_sem=block_sems.at[1],
            device_id={"seq": peer // head_count, "head": lax.rem(peer, head_count)},
            device_id_type=MESH,
        ).start()
        return 0

    lax.fori_loop(1, senders, send, 0)
    arrived[me] = staged[me]

    def locate(s, _):
        found, slot = block_for(s, seq_index)
        slot_of[s] = slot - seq_index * slot_count
        base_of[s] = (s * dev_blocks + found) * block_len
        return 0

    lax.fori_loop(0, senders, locate, 0)

    def query_rows(r):
        wide = queries[:, r].astype(jnp.float32).reshape(rows, head_dim)
        return wide.astype(jnp.bfloat16)

    def fold(carry, keys, values, valid, q):
        m, l, acc = carry
        s = lax.dot_general(keys, q, NT, preferred_element_type=jnp.float32) * scale
        s = jnp.where(valid, s, very_low)
        top = jnp.maximum(m, jnp.max(s, axis=0, keepdims=True))
        w = jnp.where(valid, jnp.exp(s - top), 0.0)
        keep = jnp.exp(m - top)
        l = l * keep + jnp.sum(w, axis=0, keepdims=True)
        acc = acc * keep + lax.dot_general(
            values, w.astype(jnp.bfloat16), TN, preferred_element_type=jnp.float32
        )
        return top, l, acc

    empty = (
        jnp.full((1, rows), very_low, jnp.float32),
        jnp.zeros((1, rows), jnp.float32),
        jnp.zeros((head_dim, rows), jnp.float32),
    )

    chunk = math.gcd(res_rows, 1024)
    for r in range(resident):
        q = query_rows(r)
        res_copies[2 * r].wait()
        res_copies[2 * r + 1].wait()
        limit = lengths[r] - seq_index * res_rows

        def step(i, carry, r=r, q=q, limit=limit):
            at = pl.ds(pl.multiple_of(i * chunk, chunk), chunk)
            valid = lax.broadcasted_iota(jnp.int32, (chunk, rows), 0) + i * chunk < limit
            return fold(carry, res_buf[0, r, at], res_buf[1, r, at], valid, q)

        m, l, acc = lax.fori_loop(0, res_rows // chunk, step, empty)
        own_stat[2 * r : 2 * r + 1] = m
        own_stat[2 * r + 1 : 2 * r + 2] = l
        own_acc[r] = acc
        pieces = acc.reshape(seq_count, part_dim, rows).astype(jnp.bfloat16)
        for z in range(seq_count):
            slice_send[z, r] = pieces[z]
        out_stat[0, 2 * r : 2 * r + 1] = m
        out_stat[0, 2 * r + 1 : 2 * r + 2] = l

    when = lax.broadcasted_iota(jnp.int32, (step_count, rows), 1) // group_size
    which = lax.broadcasted_iota(jnp.int32, (step_count, rows), 0)
    for r in range(request_count):
        allowed = which <= when
        if r >= resident:
            allowed = allowed & (which >= joined)
        m, l, acc = fold(empty, fresh[0, r], fresh[1, r], allowed, query_rows(r))
        fresh_stat[2 * r : 2 * r + 1] = m
        fresh_stat[2 * r + 1 : 2 * r + 2] = l
        fresh_acc[r] = acc

    def remote(source, target, send_sem, recv_sem, peer):
        pltpu.make_async_remote_copy(
            src_ref=source,
            dst_ref=target,
            send_sem=send_sem,
            recv_sem=recv_sem,
            device_id={"seq": peer},
            device_id_type=MESH,
        ).start()

    def drain(buffer, sem):
        part = buffer.at[pl.ds(0, seq_count - 1)]
        pltpu.make_async_copy(part, part, sem).wait()

    def push_stat(phase):
        for peer in peers:
            remote(
                out_stat.at[phase],
                got_stat.at[phase, seq_index],
                stat_send.at[phase],
                stat_recv.at[phase],
                peer,
            )

    def merge(r, phase, row, own, new, got):
        maxima = [own_stat[2 * r : 2 * r + 1], fresh_stat[2 * r : 2 * r + 1]]
        totals = [own_stat[2 * r + 1 : 2 * r + 2], fresh_stat[2 * r + 1 : 2 * r + 2]]
        for peer in peers:
            maxima.append(got_stat[phase, peer, row : row + 1])
            totals.append(got_stat[phase, peer, row + 1 : row + 2])
        top = functools.reduce(jnp.maximum, maxima)
        factors = [jnp.exp(m - top) for m in maxima]
        total = sum(f * t for f, t in zip(factors, totals))
        summed = own * factors[0] + new * factors[1]
        for peer, f in zip(peers, factors[2:]):
            summed = summed + got(peer).astype(jnp.float32) * f
        return summed / total

    push_stat(0)
    for peer in peers:
        remote(slice_send.at[peer], slice_got.at[seq_index], slice_sems.at[0], slice_sems.at[1], peer)

    drain(got_stat.at[0], stat_recv.at[0])
    drain(slice_got, slice_sems.at[1])
    mine = pl.ds(pl.multiple_of(seq_index * part_dim, part_dim), part_dim)
    for r in range(resident):
        whole_out[seq_index, r] = merge(
            r, 0, 2 * r, own_acc[r, mine], fresh_acc[r, mine], lambda peer: slice_got[peer, r]
        ).astype(jnp.bfloat16)
    for peer in peers:
        remote(
            whole_out.at[seq_index], whole_out.at[seq_index], whole_sems.at[0], whole_sems.at[1], peer
        )

    part = arrived.at[pl.ds(0, senders - 1)]
    pltpu.make_async_copy(part, part, block_sems.at[1]).wait()

    q = query_rows(resident)
    some = math.gcd(senders, 16)

    def step(i, carry):
        first = i * some
        keys = arrived[pl.ds(first, some), 0].reshape(some * block_len, head_dim)
        values = arrived[pl.ds(first, some), 1].reshape(some * block_len, head_dim)
        offsets = lax.broadcasted_iota(jnp.int32, (block_len, rows), 0)
        positions = jnp.concatenate([offsets + base_of[first + s] for s in range(some)], axis=0)
        return fold(carry, keys, values, positions < lengths[resident], q)

    m, l, acc = lax.fori_loop(0, senders // some, step, empty)
    out_acc[...] = acc.astype(jnp.bfloat16)
    out_stat[1, 0:1] = m
    out_stat[1, 1:2] = l
    own_stat[2 * resident : 2 * resident + 1] = m
    own_stat[2 * resident + 1 : 2 * resident + 2] = l
    own_acc[resident] = acc
    push_stat(1)
    for peer in peers:
        remote(out_acc, got_acc.at[seq_index], acc_send, acc_recv, peer)

    def place(j, _):
        def look(s, found):
            return jnp.where(slot_of[s] == j, s, found)

        source = lax.fori_loop(0, senders, look, jnp.int32(0), unroll=math.gcd(senders, 16))
        at = pl.ds(pl.multiple_of(j * block_len, block_len), block_len)
        for c in range(2):
            new_cache[c, 0, at] = arrived[source, c]
        return 0

    lax.fori_loop(0, slot_count, place, 0)

    def finish(r, result):
        result = jnp.transpose(result).reshape(step_count, group_size, head_dim)
        attn_out[:, r] = result.astype(jnp.bfloat16)

    drain(whole_out, whole_sems.at[1])
    for r in range(resident):
        pieces = [whole_out[z, r].astype(jnp.float32) for z in range(seq_count)]
        finish(r, jnp.concatenate(pieces, axis=0))
    drain(got_stat.at[1], stat_recv.at[1])
    drain(got_acc, acc_recv)
    r = resident
    result = merge(r, 1, 0, own_acc[r], fresh_acc[r], lambda peer: got_acc[peer])
    lane = lax.broadcasted_iota(jnp.int32, (head_dim, rows), 1) // group_size
    finish(r, jnp.where(lane >= joined, result, 0.0))

    part = staged.at[pl.ds(0, senders - 1)]
    pltpu.make_async_copy(part, part, block_sems.at[0]).wait()
    drain(got_stat.at[0], stat_send.at[0])
    drain(slice_got, slice_sems.at[0])
    drain(whole_out, whole_sems.at[0])
    drain(got_stat.at[1], stat_send.at[1])
    drain(got_acc, acc_send)


def per_device(seq_count, head_count, queries, new_kv, res_kv, prefill_kv, block_table, lengths, join_step):
    step_count, request_count, group_size, head_dim = queries.shape
    rows = step_count * group_size
    resident, res_rows = res_kv.shape[1], res_kv.shape[2]
    head_total, new_rows = prefill_kv.shape[1], prefill_kv.shape[2]
    senders = seq_count * head_count
    dev_blocks = block_table.shape[0] // senders
    block_len = new_rows // dev_blocks
    if dev_blocks != seq_count or resident > 4 or head_total != head_count:
        raise ValueError("unsupported sizes")
    slot_count = block_table.shape[0] // seq_count
    fresh = jnp.transpose(new_kv[:, :, :, 0], (0, 2, 1, 3))
    prefill = prefill_kv.reshape(2, head_total, dev_blocks, block_len, head_dim)
    part_dim = head_dim // seq_count
    out_bytes = 2 * (queries.size + 2 * slot_count * block_len * head_dim)
    vmem = pl.BlockSpec(memory_space=pltpu.VMEM)
    smem = pl.BlockSpec(memory_space=pltpu.SMEM)
    hbm = pl.BlockSpec(memory_space=pltpu.HBM)
    bf16, f32 = jnp.bfloat16, jnp.float32
    return pl.pallas_call(
        functools.partial(kernel, seq_count, head_count),
        out_shape=(
            pltpu.VMEM(queries.shape, bf16),
            pltpu.VMEM((2, 1, slot_count * block_len, head_dim), bf16),
        ),
        in_specs=[vmem, vmem, hbm, smem, smem, smem, hbm],
        out_specs=(vmem, vmem),
        scratch_shapes=[
            pltpu.VMEM(prefill.shape, bf16),
            pltpu.VMEM((2, resident, res_rows, head_dim), bf16),
            pltpu.VMEM((senders, 2, block_len, head_dim), bf16),
            pltpu.VMEM((senders, 2, block_len, head_dim), bf16),
            pltpu.VMEM((request_count, head_dim, rows), f32),
            pltpu.VMEM((16, rows), f32),
            pltpu.VMEM((request_count, head_dim, rows), f32),
            pltpu.VMEM((16, rows), f32),
            pltpu.VMEM((head_dim, rows), bf16),
            pltpu.VMEM((2, 8, rows), f32),
            pltpu.VMEM((seq_count, head_dim, rows), bf16),
            pltpu.VMEM((2, seq_count, 8, rows), f32),
            pltpu.VMEM((seq_count, resident, part_dim, rows), bf16),
            pltpu.VMEM((seq_count, resident, part_dim, rows), bf16),
            pltpu.VMEM((seq_count, resident, part_dim, rows), bf16),
            pltpu.SMEM((senders,), jnp.int32),
            pltpu.SMEM((senders,), jnp.int32),
            pltpu.SemaphoreType.DMA,
            pltpu.SemaphoreType.DMA((2, resident)),
            pltpu.SemaphoreType.DMA((2,)),
            pltpu.SemaphoreType.DMA,
            pltpu.SemaphoreType.DMA,
            pltpu.SemaphoreType.DMA((2,)),
            pltpu.SemaphoreType.DMA((2,)),
            pltpu.SemaphoreType.DMA((2,)),
            pltpu.SemaphoreType.DMA((2,)),
        ],
        compiler_params=pltpu.CompilerParams(
            collective_id=0, has_side_effects=True, vmem_limit_bytes=62 * 2**20 - 3 * out_bytes
        ),
    )(
        queries,
        fresh,
        prefill,
        block_table,
        lengths,
        join_step,
        res_kv.reshape(2, resident, res_rows, head_dim),
    )


def solution(mesh):
    in_specs = (
        P("groups", None, "head", None),
        P("groups", None, None, "head", None),
        P("groups", None, "seq", "head", None),
        P("groups", None, ("seq", "head"), None),
        P("groups"),
        P("groups"),
        P("groups"),
    )
    out_specs = (P("groups", None, "head", None), P("groups", "head", "seq", None))
    body = functools.partial(per_device, mesh.shape["seq"], mesh.shape["head"])
    return jax.shard_map(body, mesh=mesh, in_specs=in_specs, out_specs=out_specs, check_vma=False)
```
